256 devices in a mesh: gx: 8 (over z), gy: 4 (over x), gz: 8 (over y, core).
Axes of the slice: x: 4, y: 4, z: 8, core: 2. Of those that a mesh axis runs over, the one named last changes fastest.
Arguments:
- grads: float32 [256, 1, 1048576], P(('gx', 'gy', 'gz')), may hold values from -650 to 650
- loss_scale: float32 [], replicated, may hold values from 8 to 64
Outputs:
- clipped: float32 [1, 1048576], P(None, ('gx', 'gy', 'gz'))
- grad_norm: float32 [], replicated
The draws below stay inside these ranges and needn't reach their ends.
All inputs are finite; a program needn't handle non-finite values.
Results may differ from the reference program's by a relative error of at most 0.00002.
Values sent between devices are 32-bit elements; how exact they have to be, the bound alone decides.
No kernel may reach another device: no remote copies, remote signals or barrier semaphores. Data moves between devices by JAX's collectives and lax.ppermute only.
A program may use at most 64 MiB of HBM per device.

```python
import math
import jax
import jax.numpy as jnp
from jax import lax

BUCKET = 1048576
BUCKETS = 1
REPLICAS = 256


def draw_grads(key, part):
    keys = jax.random.split(jax.random.fold_in(key, 17), 3)
    columns = jnp.arange(BUCKET, dtype=jnp.float32)
    rising = jnp.sqrt(1.0 + 2.0 * columns / BUCKET)
    colscale = jnp.exp(jax.random.uniform(keys[1], (BUCKETS, BUCKET), jnp.float32) * jnp.log(10.0))
    width = BUCKET // REPLICAS
    pairing = jax.random.permutation(keys[2], REPLICAS)
    block = jnp.arange(BUCKET, dtype=jnp.int32) // width
    spike = jnp.where(block[None, None, :] == pairing[:, None, None], 6.0, 1.0)
    values = jnp.clip(jax.random.normal(keys[0], (REPLICAS, BUCKETS, BUCKET), jnp.float32), -6.0, 6.0)
    return (values * (colscale * rising)[None] * spike).astype(jnp.float32)


def setup_inputs(seed: int = 0) -> dict:
    streams_of = jax.random.split(jax.random.key(seed), 3)
    return {
        "grads": draw_grads(jax.random.fold_in(streams_of[2], 71), 0),
        "loss_scale": jnp.clip(jnp.exp(jax.random.uniform(streams_of[1], (), jnp.float32, math.log(8.0), math.log(64.0))), 8.0, 64.0),
    }


def reference(grads, loss_scale):

    def accumulate(carry, item):
        return (carry + item, None)
    total, unused = lax.scan(accumulate, jnp.zeros((BUCKETS, BUCKET), jnp.float32), grads)
    unscaled = total / loss_scale
    grad_norm = jnp.sqrt(jnp.sum(unscaled * unscaled))
    factor = jnp.minimum(1.0, 0.5 * jnp.sqrt(jnp.float32(BUCKETS * BUCKET)) / (grad_norm + 1e-06))
    return (unscaled * factor, grad_norm)
```

```python
import jax
import jax.numpy as jnp
from jax import lax
from jax.experimental import pallas as pl
from jax.experimental.pallas import tpu as pltpu
from jax.sharding import Mesh
from jax.sharding import PartitionSpec as P

Z, X, Y, CORES = 8, 4, 4, 2
DEVICES = Z * X * Y * CORES
HALF = DEVICES // CORES
ROWS, LANES = 32, 128
FIRST, SECOND = 8, 16


def device(z, x, y, core):
    return ((z * X + x) * Y + y) * CORES + core


def place(core, major, low, high, minor):
    if core == 0:
        return (2 * high + low, major, minor)
    return ((2 * high + low + 1) % Z, minor, major)


def groups(first):
    found = []
    for core in range(CORES):
        if first:
            for minor in range(4):
                for high in range(4):
                    found.append(
                        [device(*place(core, major, low, high, minor), core) for major in range(4) for low in range(2)]
                    )
        else:
            for major in range(4):
                for low in range(2):
                    found.append(
                        [device(*place(core, major, low, high, minor), core) for high in range(4) for minor in range(4)]
                    )
    return found


def copy_blocks(source, target, sem, core):
    def start(step, carry):
        major = step // 8
        low = (step // 4) % 2
        high = step % 4
        shifted = 2 * high + low

        @pl.when(core == 0)
        def _():
            pltpu.make_async_copy(source.at[shifted, major, :, 0], target.at[step], sem).start()

        @pl.when(core == 1)
        def _():
            pltpu.make_async_copy(source.at[(shifted + 1) % Z, :, major, 1], target.at[step], sem).start()

        return carry

    lax.fori_loop(0, HALF // 4, start, 0, unroll=True)
    pltpu.make_async_copy(target, target, sem).wait()


def pack(core_ref, source, target, sem):
    copy_blocks(source, target, sem, core_ref[0])


def packed(local, core):
    return pl.pallas_call(
        pack,
        out_shape=pltpu.VMEM((HALF // 4, 4, ROWS, LANES), jnp.float32),
        in_specs=[pl.BlockSpec(memory_space=pltpu.SMEM), pl.BlockSpec(memory_space=pltpu.HBM)],
        out_specs=pl.BlockSpec(memory_space=pltpu.VMEM),
        scratch_shapes=[pltpu.SemaphoreType.DMA],
        name="pack",
    )(core.reshape(1), local)


def unscale(loss_scale, parts, unscaled, squares):
    own = jnp.sum(parts[...], axis=0) / loss_scale[0]
    unscaled[...] = own
    squares[...] = jnp.broadcast_to(jnp.sum(own * own, axis=0, keepdims=True)[None], squares.shape)


def clip(unscaled, squares, clipped, norm):
    grad_norm = jnp.sqrt(jnp.sum(squares[...].reshape(DEVICES, LANES), keepdims=True))
    factor = jnp.minimum(1.0, 0.5 * jnp.sqrt(jnp.float32(DEVICES * ROWS * LANES)) / (grad_norm + 1e-06))
    clipped[...] = unscaled[...] * factor
    norm[...] = grad_norm


def per_device(grads, loss_scale):
    local = grads.reshape(Z, X, Y, CORES, ROWS, LANES)
    core = lax.axis_index("d") % CORES
    sent = packed(local, 1 - core)
    kept = packed(local, core)
    received = lax.ppermute(sent, "d", [(i, i ^ 1) for i in range(DEVICES)])
    chip = (kept + received).reshape(FIRST, SECOND * ROWS, LANES)
    first = lax.all_to_all(chip, "d", 0, 0, axis_index_groups=groups(True), tiled=True)
    first = jnp.sum(first, axis=0).reshape(SECOND, ROWS, LANES)
    second = lax.all_to_all(first, "d", 0, 0, axis_index_groups=groups(False), tiled=True)
    unscaled, squares = pl.pallas_call(
        unscale,
        out_shape=(
            jax.ShapeDtypeStruct((ROWS, LANES), jnp.float32),
            jax.ShapeDtypeStruct((DEVICES, 1, LANES), jnp.float32),
        ),
        in_specs=[pl.BlockSpec(memory_space=pltpu.SMEM), pl.BlockSpec(memory_space=pltpu.VMEM)],
        name="unscale",
    )(loss_scale.reshape(1), second)
    squares = lax.all_to_all(squares, "d", 0, 0, tiled=True)
    clipped, norm = pl.pallas_call(
        clip,
        out_shape=(
            jax.ShapeDtypeStruct((ROWS, LANES), jnp.float32),
            jax.ShapeDtypeStruct((1, 1), jnp.float32),
        ),
        name="clip",
    )(unscaled, squares)
    return (clipped.reshape(1, ROWS * LANES), norm.reshape(()))


def solution(mesh):
    flat = Mesh(mesh.devices.reshape(DEVICES), ("d",))
    return jax.shard_map(
        per_device,
        mesh=flat,
        in_specs=(P("d", None, None), P()),
        out_specs=(P(None, "d"), P()),
        check_vma=False,
    )
```

```python
import jax
import jax.numpy as jnp
from jax import lax
from jax.experimental import pallas as pl
from jax.experimental.pallas import tpu as pltpu
from jax.sharding import Mesh
from jax.sharding import PartitionSpec as P

Z, X, Y, CORES = 8, 4, 4, 2
DEVICES = Z * X * Y * CORES
HALF = DEVICES // CORES
ROWS, LANES = 32, 128
FIRST, SECOND = 8, 16


def device(z, x, y, core):
    return ((z * X + x) * Y + y) * CORES + core


def place(core, major, low, high, minor):
    if core == 0:
        return (2 * high + low, major, minor)
    return ((2 * high + low + 1) % Z, minor, major)


def groups(first):
    found = []
    for core in range(CORES):
        if first:
            for minor in range(4):
                for high in range(4):
                    found.append(
                        [device(*place(core, major, low, high, minor), core) for major in range(4) for low in range(2)]
                    )
        else:
            for major in range(4):
                for low in range(2):
                    found.append(
                        [device(*place(core, major, low, high, minor), core) for high in range(4) for minor in range(4)]
                    )
    return found


def copy_blocks(source, target, sem, partner):
    core = (lax.axis_index("d") + partner) % CORES
    for step in range(HALF // 4):
        major, low, high = (step // 8, step // 4 % 2, step % 4)
        chip = 2 * high + low

        @pl.when(core == 0)
        def _():
            pltpu.make_async_copy(source.at[chip, major, :, 0], target.at[step], sem).start()

        @pl.when(core == 1)
        def _():
            pltpu.make_async_copy(source.at[(chip + 1) % Z, :, major, 1], target.at[step], sem).start()


def pack_sent(source, sent, sem):
    copy_blocks(source, sent, sem, 1)
    pltpu.make_async_copy(sent, sent, sem).wait()


def pack_kept(loss_scale, source, kept, scale, sem):
    copy_blocks(source, kept, sem, 0)
    scale[...] = jnp.full(scale.shape, loss_scale[0])
    pltpu.make_async_copy(kept, kept, sem).wait()


def packed(local, loss_scale):
    blocks = pltpu.VMEM((HALF // 4, 4, ROWS, LANES), jnp.float32)
    in_hbm, in_smem, in_vmem = (pl.BlockSpec(memory_space=m) for m in (pltpu.HBM, pltpu.SMEM, pltpu.VMEM))
    options = dict(
        scratch_shapes=[pltpu.SemaphoreType.DMA],
        compiler_params=pltpu.CompilerParams(vmem_limit_bytes=4 << 20),
    )
    local = pltpu.with_memory_space_constraint(local, pltpu.HBM)
    sent = pl.pallas_call(
        pack_sent, out_shape=blocks, in_specs=[in_hbm], out_specs=in_vmem, name="pack_sent", **options
    )(local)
    kept, scale = pl.pallas_call(
        pack_kept,
        out_shape=(blocks, pltpu.VMEM((1, LANES), jnp.float32)),
        in_specs=[in_smem, in_hbm],
        out_specs=(in_vmem, in_vmem),
        name="pack_kept",
        **options,
    )(loss_scale, local)
    return sent, kept, scale


def unscale(scale, parts, unscaled, squares):
    own = jnp.sum(parts[...], axis=0) / scale[...]
    unscaled[...] = own
    squares[...] = jnp.broadcast_to(jnp.sum(own * own, axis=0, keepdims=True)[None], squares.shape)


def clip(unscaled, squares, clipped, norm):
    grad_norm = jnp.sqrt(jnp.sum(squares[...].reshape(DEVICES, LANES), keepdims=True))
    factor = jnp.minimum(1.0, 0.5 * jnp.sqrt(jnp.float32(DEVICES * ROWS * LANES)) / (grad_norm + 1e-06))
    clipped[...] = unscaled[...] * factor
    norm[...] = grad_norm


def per_device(grads, loss_scale):
    local = grads.reshape(Z, X, Y, CORES, ROWS, LANES)
    sent, kept, scale = packed(local, loss_scale.reshape(1))
    received = lax.ppermute(sent, "d", [(i, i ^ 1) for i in range(DEVICES)])
    chip = (kept + received).reshape(FIRST, SECOND * ROWS, LANES)
    first = lax.all_to_all(chip, "d", 0, 0, axis_index_groups=groups(True), tiled=True)
    first = jnp.sum(first, axis=0).reshape(SECOND, ROWS, LANES)
    second = lax.all_to_all(first, "d", 0, 0, axis_index_groups=groups(False), tiled=True)
    unscaled, squares = pl.pallas_call(
        unscale,
        out_shape=(
            jax.ShapeDtypeStruct((ROWS, LANES), jnp.float32),
            jax.ShapeDtypeStruct((DEVICES, 1, LANES), jnp.float32),
        ),
        compiler_params=pltpu.CompilerParams(vmem_limit_bytes=2 << 20),
        name="unscale",
    )(scale, second)
    squares = lax.all_to_all(squares, "d", 0, 0, tiled=True)
    clipped, norm = pl.pallas_call(
        clip,
        out_shape=(
            jax.ShapeDtypeStruct((ROWS, LANES), jnp.float32),
            jax.ShapeDtypeStruct((1, 1), jnp.float32),
        ),
        compiler_params=pltpu.CompilerParams(vmem_limit_bytes=2 << 20),
        name="clip",
    )(unscaled, squares)
    return (clipped.reshape(1, ROWS * LANES), norm.reshape(()))


def solution(mesh):
    flat = Mesh(mesh.devices.reshape(DEVICES), ("d",))
    return jax.shard_map(
        per_device,
        mesh=flat,
        in_specs=(P("d", None, None), P()),
        out_specs=(P(None, "d"), P()),
        check_vma=False,
    )
```

```python
import jax
import jax.numpy as jnp
from jax import lax
from jax.experimental import pallas as pl
from jax.experimental.pallas import tpu as pltpu
from jax.sharding import Mesh
from jax.sharding import PartitionSpec as P

Z, X, Y, CORES = 8, 4, 4, 2
DEVICES = Z * X * Y * CORES
HALF = DEVICES // CORES
ROWS, LANES = 32, 128
FIRST, SECOND = 8, 16


def device(z, x, y, core):
    return ((z * X + x) * Y + y) * CORES + core


def place(core, major, low, high, minor):
    if core == 0:
        return (2 * high + low, major, minor)
    return ((2 * high + low + 1) % Z, minor, major)


def groups(first):
    found = []
    for core in range(CORES):
        if first:
            for minor in range(4):
                for high in range(4):
                    found.append(
                        [device(*place(core, major, low, high, minor), core) for major in range(4) for low in range(2)]
                    )
        else:
            for major in range(4):
                for low in range(2):
                    found.append(
                        [device(*place(core, major, low, high, minor), core) for high in range(4) for minor in range(4)]
                    )
    return found


def copy_blocks(source, target, sem, partner):
    core = (lax.axis_index("d") + partner) % CORES
    for step in range(HALF // 4):
        major, low, high = (step // 8, step // 4 % 2, step % 4)
        chip = 2 * high + low

        @pl.when(core == 0)
        def _():
            pltpu.make_async_copy(source.at[chip, major, :, 0], target.at[step], sem).start()

        @pl.when(core == 1)
        def _():
            pltpu.make_async_copy(source.at[(chip + 1) % Z, :, major, 1], target.at[step], sem).start()


def pack_sent(loss_scale, source, sent, scale, sem, scale_sem, scale_smem):
    copy_blocks(source, sent, sem, 1)
    copy_scale = pltpu.make_async_copy(loss_scale, scale_smem, scale_sem)
    copy_scale.start()
    copy_scale.wait()
    scale[...] = jnp.full(scale.shape, scale_smem[0])
    pltpu.make_async_copy(sent, sent, sem).wait()


def pack_kept(source, kept, sem):
    copy_blocks(source, kept, sem, 0)
    pltpu.make_async_copy(kept, kept, sem).wait()


def packed(local, loss_scale):
    blocks = pltpu.VMEM((HALF // 4, 4, ROWS, LANES), jnp.float32)
    in_hbm, in_vmem = (pl.BlockSpec(memory_space=m) for m in (pltpu.HBM, pltpu.VMEM))
    params = pltpu.CompilerParams(vmem_limit_bytes=4 << 20)
    sem = pltpu.SemaphoreType.DMA
    local = pltpu.with_memory_space_constraint(local, pltpu.HBM)
    sent, scale = pl.pallas_call(
        pack_sent,
        out_shape=(blocks, pltpu.VMEM((1, LANES), jnp.float32)),
        in_specs=[pl.BlockSpec(memory_space=pl.ANY), in_hbm],
        out_specs=(in_vmem, in_vmem),
        scratch_shapes=[sem, sem, pltpu.SMEM((1,), jnp.float32)],
        compiler_params=params,
        name="pack_sent",
    )(loss_scale, local)
    kept = pl.pallas_call(
        pack_kept,
        out_shape=blocks,
        in_specs=[in_hbm],
        out_specs=in_vmem,
        scratch_shapes=[sem],
        compiler_params=params,
        name="pack_kept",
    )(local)
    return sent, kept, scale


def add_pair(kept, received, chip):
    chip[...] = kept[...] + received[...]


def unscale(scale, parts, unscaled, squares):
    own = jnp.sum(parts[...], axis=0) / scale[...]
    unscaled[...] = own
    squares[...] = jnp.broadcast_to(jnp.sum(own * own, axis=0, keepdims=True)[None], squares.shape)


def clip(unscaled, squares, clipped, norm):
    grad_norm = jnp.sqrt(jnp.sum(squares[...].reshape(DEVICES, LANES), keepdims=True))
    factor = jnp.minimum(1.0, 0.5 * jnp.sqrt(jnp.float32(DEVICES * ROWS * LANES)) / (grad_norm + 1e-06))
    clipped[...] = unscaled[...] * factor
    norm[...] = grad_norm


def per_device(grads, loss_scale):
    local = grads.reshape(Z, X, Y, CORES, ROWS, LANES)
    sent, kept, scale = packed(local, loss_scale.reshape(1))
    received = lax.ppermute(sent, "d", [(i, i ^ 1) for i in range(DEVICES)])
    chip = pl.pallas_call(
        add_pair,
        out_shape=pltpu.VMEM(kept.shape, jnp.float32),
        compiler_params=pltpu.CompilerParams(vmem_limit_bytes=4 << 20),
        name="add_pair",
    )(kept, pltpu.with_memory_space_constraint(received, pltpu.VMEM))
    chip = chip.reshape(FIRST, SECOND * ROWS, LANES)
    first = lax.all_to_all(chip, "d", 0, 0, axis_index_groups=groups(True), tiled=True)
    first = jnp.sum(first, axis=0).reshape(SECOND, ROWS, LANES)
    second = lax.all_to_all(first, "d", 0, 0, axis_index_groups=groups(False), tiled=True)
    unscaled, squares = pl.pallas_call(
        unscale,
        out_shape=(
            jax.ShapeDtypeStruct((ROWS, LANES), jnp.float32),
            jax.ShapeDtypeStruct((DEVICES, 1, LANES), jnp.float32),
        ),
        compiler_params=pltpu.CompilerParams(vmem_limit_bytes=2 << 20),
        name="unscale",
    )(scale, second)
    squares = lax.all_to_all(squares, "d", 0, 0, tiled=True)
    clipped, norm = pl.pallas_call(
        clip,
        out_shape=(
            jax.ShapeDtypeStruct((ROWS, LANES), jnp.float32),
            jax.ShapeDtypeStruct((1, 1), jnp.float32),
        ),
        compiler_params=pltpu.CompilerParams(vmem_limit_bytes=2 << 20),
        name="clip",
    )(unscaled, squares)
    return (clipped.reshape(1, ROWS * LANES), norm.reshape(()))


def solution(mesh):
    flat = Mesh(mesh.devices.reshape(DEVICES), ("d",))
    return jax.shard_map(
        per_device,
        mesh=flat,
        in_specs=(P("d", None, None), P()),
        out_specs=(P(None, "d"), P()),
        check_vma=False,
    )
```

```python
import jax
import jax.numpy as jnp
from jax import lax
from jax.experimental import pallas as pl
from jax.experimental.pallas import tpu as pltpu
from jax.sharding import Mesh
from jax.sharding import PartitionSpec as P

Z, X, Y, CORES = 8, 4, 4, 2
DEVICES = Z * X * Y * CORES
HALF = DEVICES // CORES
ROWS, LANES = 32, 128
PAIRS = [(i, i ^ 1) for i in range(DEVICES)]


def device(major, low, minor, high, core):
    z = 2 * high + low
    x, y = (major, minor)
    if core == 1:
        z, x, y = ((z + 1) % Z, minor, major)
    return ((z * X + x) * Y + y) * CORES + core


def along_major_and_low():
    return [
        [device(major, low, minor, high, core) for major in range(4) for low in range(2)]
        for core in range(CORES)
        for minor in range(4)
        for high in range(4)
    ]


def along_minor():
    return [
        [device(major, low, minor, high, core) for minor in range(4)]
        for core in range(CORES)
        for major in range(4)
        for low in range(2)
        for high in range(4)
    ]


def along_high():
    return [
        [device(major, low, minor, high, core) for high in range(4)]
        for core in range(CORES)
        for major in range(4)
        for low in range(2)
        for minor in range(4)
    ]


def pairs_of_planes():
    plane = X * Y * CORES
    return [list(range(2 * high * plane, 2 * (high + 1) * plane)) for high in range(4)]


def exchanged(blocks, groups):
    return lax.all_to_all(blocks, "d", 0, 0, axis_index_groups=groups, tiled=True)


def copy_blocks(source, target, sem, partner):
    core = (lax.axis_index("d") + partner) % CORES

    @pl.when(core == 0)
    def _():
        for z in range(Z):
            for x in range(X):
                pltpu.make_async_copy(source.at[z, x, :, 0], target.at[2 * x + z % 2, :, z // 2], sem).start()

    @pl.when(core == 1)
    def _():
        for z in range(Z):
            for y in range(Y):
                pltpu.make_async_copy(
                    source.at[(z + 1) % Z, :, y, 1], target.at[2 * y + z % 2, :, z // 2], sem
                ).start()


def pack_sent(loss_scale, source, sent, scale, sem, scale_sem, scale_smem):
    copy_blocks(source, sent, sem, 1)
    copy_scale = pltpu.make_async_copy(loss_scale, scale_smem, scale_sem)
    copy_scale.start()
    copy_scale.wait()
    scale[...] = jnp.full(scale.shape, scale_smem[0])
    pltpu.make_async_copy(sent, sent, sem).wait()


def pack_kept(source, kept, sem):
    copy_blocks(source, kept, sem, 0)
    pltpu.make_async_copy(kept, kept, sem).wait()


def packed(local, loss_scale):
    blocks = pltpu.VMEM((8, 4, 4, ROWS, LANES), jnp.float32)
    in_hbm, in_vmem = (pl.BlockSpec(memory_space=m) for m in (pltpu.HBM, pltpu.VMEM))
    params = pltpu.CompilerParams(vmem_limit_bytes=4 << 20)
    sem = pltpu.SemaphoreType.DMA
    local = pltpu.with_memory_space_constraint(local, pltpu.HBM)
    sent, scale = pl.pallas_call(
        pack_sent,
        out_shape=(blocks, pltpu.VMEM((1, LANES), jnp.float32)),
        in_specs=[pl.BlockSpec(memory_space=pl.ANY), in_hbm],
        out_specs=(in_vmem, in_vmem),
        scratch_shapes=[sem, sem, pltpu.SMEM((1,), jnp.float32)],
        compiler_params=params,
        name="pack_sent",
    )(loss_scale, local)
    kept = pl.pallas_call(
        pack_kept,
        out_shape=blocks,
        in_specs=[in_hbm],
        out_specs=in_vmem,
        scratch_shapes=[sem],
        compiler_params=params,
        name="pack_kept",
    )(local)
    return sent, kept, scale


def add_pair(kept, received, chip):
    chip[...] = kept[...] + received[...]


def add_minor(parts, copies):
    copies[...] = jnp.broadcast_to(jnp.sum(parts[...], axis=0, keepdims=True), copies.shape)


def unscale(scale, parts, unscaled, squares):
    index = lax.axis_index("d")
    high = (index // (X * Y * CORES) + Z - index % CORES) % Z // 2
    blocks = jnp.sum(parts[...], axis=0) / scale[...]
    unscaled[...] = jnp.sum(parts[:, pl.ds(high * ROWS, ROWS)], axis=0) / scale[...]
    squares[...] = jnp.broadcast_to(jnp.sum(blocks * blocks, axis=0, keepdims=True)[None], squares.shape)


def clip(unscaled, squares, clipped, norm):
    grad_norm = jnp.sqrt(jnp.sum(squares[...].reshape(-1, LANES), keepdims=True))
    factor = jnp.minimum(1.0, 0.5 * jnp.sqrt(jnp.float32(DEVICES * ROWS * LANES)) / (grad_norm + 1e-06))
    clipped[...] = unscaled[...] * factor
    norm[...] = grad_norm


def called(kernel, *args, out, mib=2):
    return pl.pallas_call(
        kernel,
        out_shape=out,
        compiler_params=pltpu.CompilerParams(vmem_limit_bytes=mib << 20),
        name=kernel.__name__,
    )(*args)


def per_device(grads, loss_scale):
    sent, kept, scale = packed(grads.reshape(Z, X, Y, CORES, ROWS, LANES), loss_scale.reshape(1))
    received = pltpu.with_memory_space_constraint(lax.ppermute(sent, "d", PAIRS), pltpu.VMEM)
    chip = called(add_pair, kept, received, out=pltpu.VMEM(kept.shape, jnp.float32), mib=4)
    blocks = exchanged(chip.reshape(8, 16 * ROWS, LANES), along_major_and_low())
    blocks = jnp.sum(blocks, axis=0)
    blocks = exchanged(blocks.reshape(4, 4 * ROWS, LANES), along_minor())
    copies = called(add_minor, blocks, out=pltpu.VMEM((4, 4 * ROWS, LANES), jnp.float32))
    blocks = exchanged(copies, along_high())
    unscaled, squares = called(
        unscale,
        scale,
        blocks,
        out=(
            jax.ShapeDtypeStruct((ROWS, LANES), jnp.float32),
            jax.ShapeDtypeStruct((2 * X * Y * CORES, 1, LANES), jnp.float32),
        ),
    )
    clipped, norm = called(
        clip,
        unscaled,
        exchanged(squares, pairs_of_planes()),
        out=(jax.ShapeDtypeStruct((ROWS, LANES), jnp.float32), jax.ShapeDtypeStruct((1, 1), jnp.float32)),
    )
    return (clipped.reshape(1, ROWS * LANES), norm.reshape(()))


def solution(mesh):
    flat = Mesh(mesh.devices.reshape(DEVICES), ("d",))
    return jax.shard_map(
        per_device,
        mesh=flat,
        in_specs=(P("d", None, None), P()),
        out_specs=(P(None, "d"), P()),
        check_vma=False,
    )
```

```python
import jax
import jax.numpy as jnp
from jax import lax
from jax.experimental import pallas as pl
from jax.experimental.pallas import tpu as pltpu
from jax.sharding import Mesh
from jax.sharding import PartitionSpec as P

Z, X, Y, CORES = 8, 4, 4, 2
DEVICES = Z * X * Y * CORES
HALF = DEVICES // CORES
ROWS, LANES = 32, 128
PAIRS = [(i, i ^ 1) for i in range(DEVICES)]


def device(major, low, minor, high, core):
    z = 2 * high + low
    x, y = (major, minor)
    if core == 1:
        z, x, y = ((z + 1) % Z, minor, major)
    return ((z * X + x) * Y + y) * CORES + core


def along_major_and_low():
    return [
        [device(major, low, minor, high, core) for major in range(4) for low in range(2)]
        for core in range(CORES)
        for minor in range(4)
        for high in range(4)
    ]


def along_minor():
    return [
        [device(major, low, minor, high, core) for minor in range(4)]
        for core in range(CORES)
        for major in range(4)
        for low in range(2)
        for high in range(4)
    ]


def along_high():
    return [
        [device(major, low, minor, high, core) for high in range(4)]
        for core in range(CORES)
        for major in range(4)
        for low in range(2)
        for minor in range(4)
    ]


def pairs_of_planes():
    plane = X * Y * CORES
    return [list(range(2 * high * plane, 2 * (high + 1) * plane)) for high in range(4)]


def exchanged(blocks, groups):
    return lax.all_to_all(blocks, "d", 0, 0, axis_index_groups=groups, tiled=True)


SPLIT = 2


def copy_blocks(source, target, sem, partner, first, count):
    core = (lax.axis_index("d") + partner) % CORES

    @pl.when(core == 0)
    def _():
        for at in range(first, first + count):
            for high in range(4):
                z, x = (2 * high + at % 2, at // 2)
                pltpu.make_async_copy(source.at[z, x, :, 0], target.at[at - first, :, high], sem).start()

    @pl.when(core == 1)
    def _():
        for at in range(first, first + count):
            for high in range(4):
                z, y = ((2 * high + at % 2 + 1) % Z, at // 2)
                pltpu.make_async_copy(source.at[z, :, y, 1], target.at[at - first, :, high], sem).start()


def pack_first(loss_scale, source, sent, scale, sem, scale_sem, scale_smem):
    copy_blocks(source, sent, sem, 1, 0, SPLIT)
    copy_scale = pltpu.make_async_copy(loss_scale, scale_smem, scale_sem)
    copy_scale.start()
    copy_scale.wait()
    scale[...] = jnp.full(scale.shape, scale_smem[0])
    pltpu.make_async_copy(sent, sent, sem).wait()


def pack_second(source, sent, sem):
    copy_blocks(source, sent, sem, 1, SPLIT, 8 - SPLIT)
    pltpu.make_async_copy(sent, sent, sem).wait()


def pack_kept(source, kept, sem):
    copy_blocks(source, kept, sem, 0, 0, 8)
    pltpu.make_async_copy(kept, kept, sem).wait()


def vmem_blocks(count):
    return pltpu.VMEM((count, 4, 4, ROWS, LANES), jnp.float32)


def packed(local, loss_scale):
    in_hbm, in_vmem = (pl.BlockSpec(memory_space=m) for m in (pltpu.HBM, pltpu.VMEM))
    params = pltpu.CompilerParams(vmem_limit_bytes=4 << 20)
    sem = pltpu.SemaphoreType.DMA
    local = pltpu.with_memory_space_constraint(local, pltpu.HBM)
    first, scale = pl.pallas_call(
        pack_first,
        out_shape=(vmem_blocks(SPLIT), pltpu.VMEM((1, LANES), jnp.float32)),
        in_specs=[pl.BlockSpec(memory_space=pl.ANY), in_hbm],
        out_specs=(in_vmem, in_vmem),
        scratch_shapes=[sem, sem, pltpu.SMEM((1,), jnp.float32)],
        compiler_params=params,
        name="pack_first",
    )(loss_scale, local)
    second, kept = (
        pl.pallas_call(
            kernel,
            out_shape=vmem_blocks(count),
            in_specs=[in_hbm],
            out_specs=in_vmem,
            scratch_shapes=[sem],
            compiler_params=params,
            name=kernel.__name__,
        )(local)
        for kernel, count in ((pack_second, 8 - SPLIT), (pack_kept, 8))
    )
    return first, second, kept, scale


def add_pair(kept, first, second, chip):
    chip[:SPLIT] = kept[:SPLIT] + first[...]
    chip[SPLIT:] = kept[SPLIT:] + second[...]


def add_minor(parts, copies):
    copies[...] = jnp.broadcast_to(jnp.sum(parts[...], axis=0, keepdims=True), copies.shape)


def unscale(scale, parts, unscaled, squares):
    index = lax.axis_index("d")
    high = (index // (X * Y * CORES) + Z - index % CORES) % Z // 2
    blocks = jnp.sum(parts[...], axis=0) / scale[...]
    unscaled[...] = jnp.sum(parts[:, pl.ds(high * ROWS, ROWS)], axis=0) / scale[...]
    squares[...] = jnp.broadcast_to(jnp.sum(blocks * blocks, axis=0, keepdims=True)[None], squares.shape)


def clip(unscaled, squares, clipped, norm):
    grad_norm = jnp.sqrt(jnp.sum(squares[...].reshape(-1, LANES), keepdims=True))
    factor = jnp.minimum(1.0, 0.5 * jnp.sqrt(jnp.float32(DEVICES * ROWS * LANES)) / (grad_norm + 1e-06))
    clipped[...] = unscaled[...] * factor
    norm[...] = grad_norm


def called(kernel, *args, out, mib=2):
    return pl.pallas_call(
        kernel,
        out_shape=out,
        compiler_params=pltpu.CompilerParams(vmem_limit_bytes=mib << 20),
        name=kernel.__name__,
    )(*args)


def per_device(grads, loss_scale):
    first, second, kept, scale = packed(grads.reshape(Z, X, Y, CORES, ROWS, LANES), loss_scale.reshape(1))
    received = (
        pltpu.with_memory_space_constraint(lax.ppermute(sent, "d", PAIRS), pltpu.VMEM) for sent in (first, second)
    )
    chip = called(add_pair, kept, *received, out=pltpu.VMEM(kept.shape, jnp.float32), mib=4)
    blocks = exchanged(chip.reshape(8, 16 * ROWS, LANES), along_major_and_low())
    blocks = jnp.sum(blocks, axis=0)
    blocks = exchanged(blocks.reshape(4, 4 * ROWS, LANES), along_minor())
    copies = called(add_minor, blocks, out=pltpu.VMEM((4, 4 * ROWS, LANES), jnp.float32))
    blocks = exchanged(copies, along_high())
    unscaled, squares = called(
        unscale,
        scale,
        blocks,
        out=(
            jax.ShapeDtypeStruct((ROWS, LANES), jnp.float32),
            jax.ShapeDtypeStruct((2 * X * Y * CORES, 1, LANES), jnp.float32),
        ),
    )
    clipped, norm = called(
        clip,
        unscaled,
        exchanged(squares, pairs_of_planes()),
        out=(jax.ShapeDtypeStruct((ROWS, LANES), jnp.float32), jax.ShapeDtypeStruct((1, 1), jnp.float32)),
    )
    return (clipped.reshape(1, ROWS * LANES), norm.reshape(()))


def solution(mesh):
    flat = Mesh(mesh.devices.reshape(DEVICES), ("d",))
    return jax.shard_map(
        per_device,
        mesh=flat,
        in_specs=(P("d", None, None), P()),
        out_specs=(P(None, "d"), P()),
        check_vma=False,
    )
```

```python
import jax
import jax.numpy as jnp
from jax import lax
from jax.experimental import pallas as pl
from jax.experimental.pallas import tpu as pltpu
from jax.sharding import Mesh
from jax.sharding import PartitionSpec as P

Z, X, Y, CORES = 8, 4, 4, 2
DEVICES = Z * X * Y * CORES
ROWS, LANES = 32, 128
PAIRS = [(i, i ^ 1) for i in range(DEVICES)]


def device(major, low, minor, high, core):
    z = 2 * high + low
    x, y = (major, minor)
    if core == 1:
        z, x, y = ((z + 1) % Z, minor, major)
    return ((z * X + x) * Y + y) * CORES + core


def along_major_and_low():
    return [
        [device(major, low, minor, high, core) for major in range(4) for low in range(2)]
        for core in range(CORES)
        for minor in range(4)
        for high in range(4)
    ]


def along_minor():
    return [
        [device(major, low, minor, high, core) for minor in range(4)]
        for core in range(CORES)
        for major in range(4)
        for low in range(2)
        for high in range(4)
    ]


def along_high():
    return [
        [device(major, low, minor, high, core) for high in range(4)]
        for core in range(CORES)
        for major in range(4)
        for low in range(2)
        for minor in range(4)
    ]


def pairs_of_planes():
    plane = X * Y * CORES
    return [list(range(2 * high * plane, 2 * (high + 1) * plane)) for high in range(4)]


def exchanged(blocks, groups):
    return lax.all_to_all(blocks, "d", 0, 0, axis_index_groups=groups, tiled=True)


def staying(core):
    index = lax.axis_index("d")
    x, y, z = (index // (Y * CORES) % X, index // CORES % Y, index // (X * Y * CORES))
    return 2 * jnp.where(core == 0, x, y) + (z + core) % 2


def copy_chunk(source, target, sem, core, own, at):
    @pl.when(core == own)
    def _():
        for high in range(4):
            z = (2 * high + at % 2 + own) % Z
            blocks = source.at[z, at // 2, :, 0] if own == 0 else source.at[z, :, at // 2, 1]
            pltpu.make_async_copy(blocks, target.at[:, high], sem).start()


def copy_sent(source, sent, sem, first):
    core = 1 - lax.axis_index("d") % CORES
    for k in range(sent.shape[0]):
        at = (staying(core) + first + k) % 8
        for own in range(CORES):
            copy_chunk(source, sent.at[k], sem, core, own, at)


def pack_first(source, sent, sem):
    copy_sent(source, sent, sem, 1)
    pltpu.make_async_copy(sent, sent, sem).wait()


def pack_rest(loss_scale, source, sent, last, kept, scale, sem, last_sem, kept_sem, scale_sem, scale_smem):
    copy_sent(source, sent, sem, 7)
    copy_sent(source, last, last_sem, 0)
    core = lax.axis_index("d") % CORES
    for at in range(8):
        for own in range(CORES):
            copy_chunk(source, kept.at[at], kept_sem, core, own, at)
    copy_scale = pltpu.make_async_copy(loss_scale, scale_smem, scale_sem)
    copy_scale.start()
    copy_scale.wait()
    scale[...] = jnp.full(scale.shape, scale_smem[0])
    pltpu.make_async_copy(sent, sent, sem).wait()
    pltpu.make_async_copy(last, last, last_sem).wait()
    pltpu.make_async_copy(kept, kept, kept_sem).wait()


def vmem_blocks(count):
    return pltpu.VMEM((count, 4, 4, ROWS, LANES), jnp.float32)


def packed(local, loss_scale):
    in_hbm, in_vmem = (pl.BlockSpec(memory_space=m) for m in (pltpu.HBM, pltpu.VMEM))
    params = pltpu.CompilerParams(vmem_limit_bytes=4 << 20)
    sem = pltpu.SemaphoreType.DMA
    local = pltpu.with_memory_space_constraint(local, pltpu.HBM)
    def copied(kernel, count):
        return pl.pallas_call(
            kernel,
            out_shape=vmem_blocks(count),
            in_specs=[in_hbm],
            out_specs=in_vmem,
            scratch_shapes=[sem],
            compiler_params=params,
        )(local)

    first = copied(pack_first, 6)
    rest, last, kept, scale = pl.pallas_call(
        pack_rest,
        out_shape=(vmem_blocks(1), vmem_blocks(1), vmem_blocks(8), pltpu.VMEM((1, LANES), jnp.float32)),
        in_specs=[pl.BlockSpec(memory_space=pl.ANY), in_hbm],
        out_specs=(in_vmem, in_vmem, in_vmem, in_vmem),
        scratch_shapes=[sem, sem, sem, sem, pltpu.SMEM((1,), jnp.float32)],
        compiler_params=params,
        name="pack_rest",
    )(loss_scale, local)
    return first, rest, last, kept, scale


def add_pair(kept, first, rest, chip):
    stays = staying(lax.axis_index("d") % CORES)
    chip[stays] = kept[stays]
    for k in range(1, 8):
        at = (stays + k) % 8
        chip[at] = kept[at] + (first[k - 1] if k < 7 else rest[0])


def add_eight(parts, total):
    total[...] = jnp.sum(parts[...], axis=0)


def add_last(total, last, blocks):
    blocks[...] = total[...] + last[...]


def add_minor(parts, copies):
    copies[...] = jnp.broadcast_to(jnp.sum(parts[...], axis=0, keepdims=True), copies.shape)


def unscale(scale, parts, unscaled, squares):
    index = lax.axis_index("d")
    high = (index // (X * Y * CORES) + Z - index % CORES) % Z // 2
    blocks = jnp.sum(parts[...], axis=0) / scale[...]
    unscaled[...] = jnp.sum(parts[:, pl.ds(high * ROWS, ROWS)], axis=0) / scale[...]
    squares[...] = jnp.broadcast_to(jnp.sum(blocks * blocks, axis=0, keepdims=True)[None], squares.shape)


def clip(unscaled, squares, clipped, norm):
    grad_norm = jnp.sqrt(jnp.sum(squares[...].reshape(-1, LANES), keepdims=True))
    factor = jnp.minimum(1.0, 0.5 * jnp.sqrt(jnp.float32(DEVICES * ROWS * LANES)) / (grad_norm + 1e-06))
    clipped[...] = unscaled[...] * factor
    norm[...] = grad_norm


def called(kernel, *args, out, mib=2):
    return pl.pallas_call(
        kernel, out_shape=out, compiler_params=pltpu.CompilerParams(vmem_limit_bytes=mib << 20)
    )(*args)


def per_device(grads, loss_scale):
    *sent, kept, scale = packed(grads.reshape(Z, X, Y, CORES, ROWS, LANES), loss_scale.reshape(1))
    first, rest = (lax.ppermute(chunks, "d", PAIRS) for chunks in sent[:2])
    last = lax.ppermute(sent[2], "d", PAIRS)
    first, rest = (pltpu.with_memory_space_constraint(a, pltpu.VMEM) for a in (first, rest))
    chip = called(add_pair, kept, first, rest, out=pltpu.VMEM(kept.shape, jnp.float32), mib=4)
    blocks = exchanged(chip.reshape(8, 16 * ROWS, LANES), along_major_and_low())
    blocks = called(add_eight, blocks, out=pltpu.VMEM((16 * ROWS, LANES), jnp.float32))
    last = last.reshape(16 * ROWS, LANES)
    blocks = called(add_last, blocks, last, out=pltpu.VMEM((16 * ROWS, LANES), jnp.float32))
    blocks = exchanged(blocks.reshape(4, 4 * ROWS, LANES), along_minor())
    copies = called(add_minor, blocks, out=pltpu.VMEM((4, 4 * ROWS, LANES), jnp.float32))
    blocks = exchanged(copies, along_high())
    unscaled, squares = called(
        unscale,
        scale,
        blocks,
        out=(
            jax.ShapeDtypeStruct((ROWS, LANES), jnp.float32),
            jax.ShapeDtypeStruct((2 * X * Y * CORES, 1, LANES), jnp.float32),
        ),
    )
    clipped, norm = called(
        clip,
        unscaled,
        exchanged(squares, pairs_of_planes()),
        out=(jax.ShapeDtypeStruct((ROWS, LANES), jnp.float32), jax.ShapeDtypeStruct((1, 1), jnp.float32)),
    )
    return (clipped.reshape(1, ROWS * LANES), norm.reshape(()))


def solution(mesh):
    flat = Mesh(mesh.devices.reshape(DEVICES), ("d",))
    return jax.shard_map(
        per_device,
        mesh=flat,
        in_specs=(P("d", None, None), P()),
        out_specs=(P(None, "d"), P()),
        check_vma=False,
    )
```
